32 devices in a mesh: row: 8 (over y, x, core), col: 4 (over z).
Axes of the slice: x: 2, y: 2, z: 4, core: 2. Of those that a mesh axis runs over, the one named last changes fastest.
Arguments:
- observed: float32 [1024, 2048], P('row', 'col'), may hold values from -6 to 6
- psf_table: bfloat16 [64, 31, 31], replicated, may hold values from 0.049804688 to 1
- psf_index: int32 [8, 16], P('row', 'col'), may hold values from 0 to 63
- start_image: float32 [1024, 2048], P('row', 'col'), may hold values from -6 to 6
- blur_dual: float32 [1024, 2048], P('row', 'col'), may hold values from -6 to 6
- tv_dual: float32 [2, 1024, 2048], P(None, 'row', 'col'), may hold values from -1.8 to 1.8
Outputs:
- restored: float32 [1024, 2048], P('row', 'col')
- blur_dual_out: float32 [1024, 2048], P('row', 'col')
The draws below stay inside these ranges and needn't reach their ends.
Inputs may be any that keep to these rules, and one draw needn't show every extreme that they name: `psf_index`: each entry names a row of psf_table.
All inputs are finite; a program needn't handle non-finite values.
Results may differ from the reference program's by a relative error of at most 0.0003.
Values may be sent and summed in bfloat16 or wider, within the bound.
A program may use at most 128 MiB of HBM per device.

```python
import math
import jax
import jax.numpy as jnp
from jax import lax

KS = 31
PR = 128
PC = 128
NPSF = 64
ITERS = 2
NX = 1024
NY = 2048
NPC = 16
N_ROW = 8


def plant(values, own_key, low, high):
    spot = [jax.random.randint(jax.random.fold_in(own_key, axis), (), 0, length) for axis, length in enumerate(values.shape)]
    widest = values.shape.index(max(values.shape))
    neighbour = spot[:widest] + [(spot[widest] + 1) % values.shape[widest]] + spot[widest + 1:]
    return values.at[tuple(spot)].set(low).at[tuple(neighbour)].set(high)


def steps_of(own_key, extent, split, low, largest):
    level = 1.0
    for position, parts in split:
        steps = jax.random.uniform(jax.random.fold_in(jax.random.fold_in(own_key, 6), position), (parts,), jnp.float32, low / len(split), largest / len(split))
        level = level * jnp.repeat(jnp.exp(steps), extent[position] // parts).reshape((-1,) + (1,) * (len(extent) - 1 - position))
    return level


def noise(rng, shape, scale, limit, split=(), kind=jnp.bfloat16):
    factor_of = steps_of(rng, shape, split, -0.22, 0.18) if split else 1.0
    array = jax.random.normal(rng, shape, jnp.float32) * scale * factor_of
    return jnp.minimum(jnp.maximum(array, -limit), limit).astype(kind)


def setup_inputs(seed: int = 0) -> dict:
    key_of = jax.random.split(jax.random.key(seed), 7)
    observed = noise(key_of[0], (NX, NY), 1.0, 6.0, ((0, 8), (1, 4)), jnp.float32)
    psf_table = jnp.clip(jnp.exp(jax.random.uniform(key_of[1], (NPSF, KS, KS), jnp.float32, math.log(0.049804688), math.log(1.0))), 0.049804688, 1.0).astype(jnp.bfloat16)
    psf_index = plant(jax.random.randint(key_of[2], (N_ROW, NPC), 0, NPSF), jax.random.fold_in(key_of[2], 1), 0, NPSF - 1).astype(jnp.int32)
    start_image = noise(key_of[3], (NX, NY), 1.0, 6.0, ((0, 8), (1, 4)), jnp.float32)
    blur_dual = noise(key_of[4], (NX, NY), 1.0, 6.0, ((0, 8), (1, 4)), jnp.float32)
    tv_dual = noise(key_of[5], (2, NX, NY), 0.3, 1.8, ((1, 8), (2, 4)), jnp.float32)
    return {"observed": observed, "psf_table": psf_table, "psf_index": psf_index, "start_image": start_image, "blur_dual": blur_dual, "tv_dual": tv_dual}


sigma_step = 0.15
tau_step = 0.6
tv_weight = 0.5
group_size = 4

def make_select(kernel_size, patch_cols):
    half_width = kernel_size // 2
    column_in = jnp.arange(patch_cols + 2 * half_width, dtype=jnp.int32)[None, :, None]
    column_out = jnp.arange(patch_cols, dtype=jnp.int32)[None, None, :]
    tap_index = jnp.arange(kernel_size, dtype=jnp.int32)[:, None, None]
    return (column_in - column_out == tap_index).astype(jnp.float32)

def strip_pass(strip_in, observed_s, dual_s, index_s, kern_flat, select):
    kernel_size = select.shape[0]
    patch_cols = select.shape[2]
    half_width = (select.shape[1] - patch_cols) // 2
    patch_rows, width = observed_s.shape
    group_span = group_size * patch_cols
    group_count = width // group_span
    table_size = kern_flat.shape[0]

    def one_group(spread_sum, group_id):
        first_col = group_id * group_span
        window = lax.dynamic_slice_in_dim(strip_in, first_col, group_span + 2 * half_width, 1)
        pieces = jnp.stack([window[:, member * patch_cols:member * patch_cols + patch_cols + 2 * half_width] for member in range(group_size)])
        stacked = jnp.stack([pieces[:, tap_row:tap_row + patch_rows, :] for tap_row in range(kernel_size)], axis=2)
        patch_ids = lax.dynamic_slice_in_dim(index_s, group_id * group_size, group_size)
        onehot = (patch_ids[:, None] == jnp.arange(table_size, dtype=jnp.int32)[None, :]).astype(jnp.float32)
        kernels = jnp.dot(onehot, kern_flat, precision=lax.Precision.HIGHEST).reshape(group_size, kernel_size, kernel_size)
        toeplitz = jnp.einsum('pab,bkj->pakj', kernels, select, precision=lax.Precision.HIGHEST)
        blurred = jnp.einsum('piak,pakj->pij', stacked, toeplitz, precision=lax.Precision.HIGHEST)
        blurred = blurred.transpose(1, 0, 2).reshape(patch_rows, group_span)
        seen_group = lax.dynamic_slice_in_dim(observed_s, first_col, group_span, 1)
        dual_group = lax.dynamic_slice_in_dim(dual_s, first_col, group_span, 1)
        dual_new = (dual_group + sigma_step * (blurred - seen_group)) / (1.0 + sigma_step)
        rounded = lax.optimization_barrier(dual_new.astype(jnp.bfloat16)).astype(jnp.float32)
        rounded = rounded.reshape(patch_rows, group_size, patch_cols).transpose(1, 0, 2)
        padded_dual = jnp.pad(rounded, ((0, 0), (kernel_size - 1, kernel_size - 1), (0, 0)))
        shifted = jnp.stack([padded_dual[:, kernel_size - 1 - tap_row:kernel_size - 1 - tap_row + patch_rows + 2 * half_width, :] for tap_row in range(kernel_size)], axis=2)
        spread = jnp.einsum('praj,pakj->prk', shifted, toeplitz, precision=lax.Precision.HIGHEST)
        merged = jnp.zeros((patch_rows + 2 * half_width, group_span + 2 * half_width), jnp.float32)
        for member in range(group_size):
            merged = merged.at[:, member * patch_cols:member * patch_cols + patch_cols + 2 * half_width].add(spread[member])
        previous = lax.dynamic_slice_in_dim(spread_sum, first_col, group_span + 2 * half_width, 1)
        spread_sum = lax.dynamic_update_slice_in_dim(spread_sum, previous + merged, first_col, 1)
        return (spread_sum, dual_new)
    start_sum = jnp.zeros((patch_rows + 2 * half_width, width + 2 * half_width), jnp.float32)
    spread_sum, duals = lax.scan(one_group, start_sum, jnp.arange(group_count, dtype=jnp.int32))
    return (duals.transpose(1, 0, 2).reshape(patch_rows, width), spread_sum)

def reference(observed, psf_table, psf_index, start_image, blur_dual, tv_dual):
    half_width = KS // 2
    table = psf_table.astype(jnp.float32)
    normed = table / lax.optimization_barrier(jnp.sum(table, axis=(1, 2), keepdims=True))
    kern_flat = lax.optimization_barrier(normed.astype(jnp.bfloat16)).astype(jnp.float32).reshape(NPSF, KS * KS)
    select = make_select(KS, PC)
    restored = start_image
    extrapolated = start_image
    dual_now = blur_dual
    tv_rows = tv_dual[0]
    tv_cols = tv_dual[1]
    keep_rows = (jnp.arange(NX, dtype=jnp.int32) < NX - 1)[:, None]
    keep_cols = (jnp.arange(NY, dtype=jnp.int32) < NY - 1)[None, :]
    for step in range(ITERS):
        padded = lax.optimization_barrier(jnp.pad(extrapolated, half_width).astype(jnp.bfloat16)).astype(jnp.float32)

        def one_strip(carry, strip_id):
            start_row = strip_id * PR
            strip_in = lax.dynamic_slice_in_dim(padded, start_row, PR + 2 * half_width, 0)
            seen_strip = lax.dynamic_slice_in_dim(observed, start_row, PR, 0)
            dual_strip = lax.dynamic_slice_in_dim(dual_now, start_row, PR, 0)
            index_strip = lax.dynamic_index_in_dim(psf_index, strip_id, 0, keepdims=False)
            new_dual, spread_sum = strip_pass(strip_in, seen_strip, dual_strip, index_strip, kern_flat, select)
            return (carry, (new_dual, spread_sum))
        unused, (dual_strips, spread_strips) = lax.scan(one_strip, jnp.zeros((), jnp.float32), jnp.arange(N_ROW, dtype=jnp.int32))
        dual_now = dual_strips.reshape(NX, NY)

        def add_strip(strip_id, total):
            piece = spread_strips[strip_id]
            start_row = (strip_id * PR).astype(jnp.int32)
            zero_col = jnp.zeros((), jnp.int32)
            previous = lax.dynamic_slice(total, (start_row, zero_col), piece.shape)
            return lax.dynamic_update_slice(total, previous + piece, (start_row, zero_col))
        total = lax.fori_loop(0, N_ROW, add_strip, jnp.zeros((NX + 2 * half_width, NY + 2 * half_width), jnp.float32))
        adjoint = total[half_width:half_width + NX, half_width:half_width + NY]
        below = jnp.concatenate([extrapolated[1:], jnp.zeros((1, NY), jnp.float32)], axis=0)
        right = jnp.concatenate([extrapolated[:, 1:], jnp.zeros((NX, 1), jnp.float32)], axis=1)
        grad_rows = jnp.where(keep_rows, below - extrapolated, 0.0)
        grad_cols = jnp.where(keep_cols, right - extrapolated, 0.0)
        moved_rows = tv_rows + sigma_step * grad_rows
        moved_cols = tv_cols + sigma_step * grad_cols
        shrink = jnp.maximum(1.0, jnp.sqrt(moved_rows * moved_rows + moved_cols * moved_cols) / tv_weight)
        tv_rows = moved_rows / shrink
        tv_cols = moved_cols / shrink
        masked_rows = jnp.where(keep_rows, tv_rows, 0.0)
        masked_cols = jnp.where(keep_cols, tv_cols, 0.0)
        diverge = masked_rows - jnp.concatenate([jnp.zeros((1, NY), jnp.float32), masked_rows[:-1]], axis=0)
        diverge = diverge + masked_cols - jnp.concatenate([jnp.zeros((NX, 1), jnp.float32), masked_cols[:, :-1]], axis=1)
        next_image = restored - tau_step * (adjoint - diverge)
        extrapolated = 2.0 * next_image - restored
        restored = next_image
    return (restored, dual_now)
```

```python
import functools

import jax
import jax.numpy as jnp
from jax import lax
from jax.experimental import pallas as pl
from jax.experimental.pallas import tpu as pltpu
from jax.sharding import PartitionSpec as P

ITERS = 2
SIGMA = 0.15
TAU = 0.6
TV_WEIGHT = 0.5
LANES = 128
GROUP = 16
MESH = pl.DeviceIdType.MESH

DIRECTIONS = ((-1, 0), (1, 0), (0, -1), (0, 1), (-1, -1), (-1, 1), (1, -1), (1, 1))
UP, DOWN, LEFT, RIGHT, UP_LEFT, UP_RIGHT, DOWN_LEFT, DOWN_RIGHT = range(8)
OPPOSITE = (DOWN, UP, RIGHT, LEFT, DOWN_RIGHT, DOWN_LEFT, UP_RIGHT, UP_LEFT)


def body(
    kernel_size,
    index_ref,
    observed_ref,
    table_ref,
    start_ref,
    dual_ref,
    tv_ref,
    restored_ref,
    dual_out_ref,
    taps,
    taps_back,
    weights,
    weights_rest,
    adjoint,
    adjoint_rest,
    stack,
    padded_dual,
    bars,
    sums,
    image,
    tv,
    got_rows,
    got_cols,
    got_corners,
    send_sem,
    recv_sem,
):
    half = kernel_size // 2
    rows, cols = observed_ref.shape
    patches = index_ref.shape[1]
    tiles = patches + 1
    wide = tiles * LANES
    tall = rows + 2 * GROUP
    reach = rows + GROUP
    last = wide - LANES
    row, col = lax.axis_index("row"), lax.axis_index("col")
    row_count, col_count = lax.axis_size("row"), lax.axis_size("col")

    def there(d):
        r, c = row + DIRECTIONS[d][0], col + DIRECTIONS[d][1]
        return (r >= 0) & (r < row_count) & (c >= 0) & (c < col_count)

    def device(d):
        return (row + DIRECTIONS[d][0], col + DIRECTIONS[d][1])

    got_rows[...] = jnp.zeros_like(got_rows)
    got_cols[...] = jnp.zeros_like(got_cols)
    got_corners[...] = jnp.zeros_like(got_corners)

    barrier = pltpu.get_barrier_semaphore()
    for d in range(8):

        @pl.when(there(d))
        def _():
            pl.semaphore_signal(barrier, inc=1, device_id=device(d), device_id_type=MESH)

    lane = lax.broadcasted_iota(jnp.int32, (1, LANES), 1)
    lane_wide = lax.broadcasted_iota(jnp.int32, (1, wide), 1)
    row_id = lax.broadcasted_iota(jnp.int32, (rows, 1), 0)
    own_lane = (lane_wide >= half) & (lane_wide < half + cols)
    keep_rows = (row_id < rows - 1) | (row < row_count - 1)
    keep_cols = (lane_wide < half + cols - 1) | (col < col_count - 1)

    def shifted(value):
        full = jnp.concatenate([value, jnp.zeros((rows, LANES), jnp.float32)], axis=1)
        return pltpu.roll(full, half, axis=1)

    start = shifted(start_ref[...])
    image[...] = start
    bars[0, :GROUP, :] = jnp.zeros((GROUP, wide), jnp.float32)
    bars[0, GROUP : GROUP + rows, :] = start
    bars[0, GROUP + rows :, :] = jnp.zeros((GROUP, wide), jnp.float32)

    tall_peers = (row > 0).astype(jnp.int32) + (row < row_count - 1).astype(jnp.int32)
    wide_peers = (col > 0).astype(jnp.int32) + (col < col_count - 1).astype(jnp.int32)
    pl.semaphore_wait(barrier, (tall_peers + 1) * (wide_peers + 1) - 1)

    inner = pl.ds(GROUP, rows)

    def copies(turn, source, low, high):
        row_part = {-1: low, 0: inner, 1: high}
        col_part = {-1: pl.ds(0, LANES), 0: pl.ds(0, wide), 1: pl.ds(last, LANES)}
        result = []
        for d, (dr, dc) in enumerate(DIRECTIONS):
            back = OPPOSITE[d]
            if d in (UP, DOWN):
                target = got_rows.at[turn, back - UP]
            elif d in (LEFT, RIGHT):
                target = got_cols.at[turn, back - LEFT]
            else:
                target = got_corners.at[turn, back - UP_LEFT]
            send = pltpu.make_async_remote_copy(
                src_ref=source.at[row_part[dr], col_part[dc]],
                dst_ref=target,
                send_sem=send_sem.at[turn, d],
                recv_sem=recv_sem.at[turn, back],
                device_id=device(d),
                device_id_type=MESH,
            )
            arrive = pltpu.make_async_remote_copy(
                src_ref=source.at[row_part[dr], col_part[dc]],
                dst_ref=(
                    got_rows.at[turn, d - UP]
                    if d in (UP, DOWN)
                    else got_cols.at[turn, d - LEFT]
                    if d in (LEFT, RIGHT)
                    else got_corners.at[turn, d - UP_LEFT]
                ),
                send_sem=send_sem.at[turn, d],
                recv_sem=recv_sem.at[turn, d],
                device_id=device(d),
                device_id_type=MESH,
            )
            result.append((send, arrive))
        return result

    def start_copies(made):
        for d in (LEFT, RIGHT, UP, DOWN, UP_LEFT, UP_RIGHT, DOWN_LEFT, DOWN_RIGHT):

            @pl.when(there(d))
            def _():
                made[d][0].start()

    def wait_copies(made):
        for d in range(8):

            @pl.when(there(d))
            def _():
                made[d][0].wait_send()
                made[d][1].wait_recv()

    image_low, image_high = pl.ds(GROUP, GROUP), pl.ds(rows, GROUP)
    sums_low, sums_high = pl.ds(0, GROUP), pl.ds(GROUP + rows, GROUP)

    exchange = copies(0, bars.at[0], image_low, image_high)
    start_copies(exchange)

    tv[0] = shifted(tv_ref[0])
    tv[1] = shifted(tv_ref[1])
    dual_out_ref[...] = dual_ref[...]
    padded_dual[...] = jnp.zeros_like(padded_dual)
    taps[...] = jnp.zeros_like(taps)
    turned = lax.broadcasted_iota(jnp.int32, (LANES, LANES), 0)
    column = lax.broadcasted_iota(jnp.int32, (LANES, LANES), 1)
    reverse = (((turned + column) == LANES) | ((turned + column) == 0)).astype(jnp.bfloat16)
    for patch in range(patches):
        entry = table_ref[index_ref[0, patch]].astype(jnp.float32)
        normed = (entry / jnp.sum(entry)).astype(jnp.bfloat16).astype(jnp.float32)
        taps[patch, :kernel_size, :kernel_size] = normed
        taps_back[patch] = jnp.dot(
            taps[patch].astype(jnp.bfloat16), reverse, preferred_element_type=jnp.float32
        )

    def circulant(base):
        return pltpu.roll(
            jnp.broadcast_to(base, (LANES, LANES)), 0, axis=1, stride=1, stride_axis=0
        )

    below_diagonal = column <= turned
    above_diagonal = column >= turned

    def build(step, carry):
        patch = step // GROUP
        shift = step % GROUP
        here = pl.ds(pl.multiple_of(shift * LANES, LANES), LANES)
        for n in range(2):
            span = pl.ds(n * LANES, LANES)
            base = taps_back[patch, pl.ds(n * GROUP + shift, 1), :]
            full = circulant(base)
            weights[patch, here, span] = jnp.where(below_diagonal, full, 0.0).astype(jnp.bfloat16)
            weights_rest[patch, here, span] = jnp.where(below_diagonal, 0.0, full).astype(
                jnp.bfloat16
            )
            base = taps[patch, pl.ds(n * GROUP + GROUP - 1 - shift, 1), :]
            full = circulant(base)
            adjoint[patch, here, span] = jnp.where(above_diagonal, full, 0.0).astype(jnp.bfloat16)
            adjoint_rest[patch, here, span] = jnp.where(above_diagonal, 0.0, full).astype(
                jnp.bfloat16
            )
        return carry

    lax.fori_loop(0, patches * GROUP, build, 0)

    wait_copies(exchange)

    for step in range(ITERS):
        turn = 2 * step
        bar = bars.at[step]
        total = sums.at[step]

        middle = pl.ds(GROUP, rows)
        tile_first, tile_last = pl.ds(0, LANES), pl.ds(last, LANES)
        in_left = lane < half
        bar[middle, tile_first] = jnp.where(in_left, got_cols[turn, 0], bar[middle, tile_first])
        bar[middle, tile_last] = jnp.where(in_left, bar[middle, tile_last], got_cols[turn, 1])
        for side, place in ((0, pl.ds(0, GROUP)), (1, pl.ds(GROUP + rows, GROUP))):
            bar[place, :] = got_rows[turn, side]
            bar[place, tile_first] = jnp.where(
                in_left, got_corners[turn, 2 * side], got_rows[turn, side, :, :LANES]
            )
            bar[place, tile_last] = jnp.where(
                in_left, got_rows[turn, side, :, last:], got_corners[turn, 2 * side + 1]
            )

        def stack_bar(tile, carry):
            here = pl.ds(pl.multiple_of(tile * LANES, LANES), LANES)
            for shift in range(GROUP):
                stack[tile, :, shift * LANES : (shift + 1) * LANES] = bar[
                    pl.ds(shift + 1, reach), here
                ].astype(jnp.bfloat16)
            return carry

        lax.fori_loop(0, tiles, stack_bar, 0)

        def blur(patch, carry):
            here = pl.ds(pl.multiple_of(patch * LANES, LANES), LANES)
            both = jnp.dot(stack[patch], weights[patch], preferred_element_type=jnp.float32)
            both += jnp.dot(
                stack[patch + 1], weights_rest[patch], preferred_element_type=jnp.float32
            )
            blurred = both[:rows, :LANES] + both[GROUP:, LANES:]
            dual = (dual_out_ref[:, here] + SIGMA * (blurred - observed_ref[:, here])) / (
                1.0 + SIGMA
            )
            dual_out_ref[:, here] = dual
            padded_dual[GROUP : GROUP + rows, here] = dual
            return carry

        lax.fori_loop(0, patches, blur, 0)

        def stack_dual(patch, carry):
            here = pl.ds(pl.multiple_of(patch * LANES, LANES), LANES)
            for shift in range(GROUP):
                stack[patch, :, shift * LANES : (shift + 1) * LANES] = padded_dual[
                    pl.ds(shift, reach), here
                ].astype(jnp.bfloat16)
            return carry

        lax.fori_loop(0, patches, stack_dual, 0)

        def put(tile, both):
            here = pl.ds(pl.multiple_of(tile * LANES, LANES), LANES)
            total[:GROUP, here] = both[:GROUP, :LANES]
            total[pl.ds(GROUP, rows), here] = both[GROUP:, :LANES] + both[:rows, LANES:]
            total[pl.ds(GROUP + rows, GROUP), here] = both[rows:, LANES:]

        put(0, jnp.dot(stack[0], adjoint[0], preferred_element_type=jnp.float32))

        def spread(tile, carry):
            both = jnp.dot(stack[tile], adjoint[tile], preferred_element_type=jnp.float32)
            both += jnp.dot(
                stack[tile - 1], adjoint_rest[tile - 1], preferred_element_type=jnp.float32
            )
            put(tile, both)
            return carry

        lax.fori_loop(1, patches, spread, 0)
        put(
            patches,
            jnp.dot(
                stack[patches - 1], adjoint_rest[patches - 1], preferred_element_type=jnp.float32
            ),
        )

        now = bar[middle, :]
        grad_rows = jnp.where(keep_rows, bar[pl.ds(GROUP + 1, rows), :] - now, 0.0)
        grad_cols = jnp.where(keep_cols, pltpu.roll(now, wide - 1, axis=1) - now, 0.0)
        moved_rows = tv[0] + SIGMA * grad_rows
        moved_cols = tv[1] + SIGMA * grad_cols
        shrink = jnp.maximum(
            1.0, jnp.sqrt(moved_rows * moved_rows + moved_cols * moved_cols) / TV_WEIGHT
        )
        new_rows = moved_rows / shrink
        new_cols = moved_cols / shrink
        tv[0] = new_rows
        tv[1] = new_cols
        masked_rows = jnp.where(keep_rows & own_lane, new_rows, 0.0)
        masked_cols = jnp.where(keep_cols & own_lane, new_cols, 0.0)
        total[middle, :] += pltpu.roll(masked_cols, 1, axis=1) - masked_cols - masked_rows
        total[pl.ds(GROUP + 1, rows), :] += masked_rows

        exchange = copies(turn + 1, total, sums_low, sums_high)
        start_copies(exchange)
        wait_copies(exchange)

        got = turn + 1
        total[middle, tile_first] += got_cols[got, 0]
        total[middle, tile_last] += got_cols[got, 1]
        for side, place in ((0, pl.ds(GROUP, GROUP)), (1, pl.ds(rows, GROUP))):
            total[place, :] += got_rows[got, side]
            total[place, tile_first] += got_corners[got, 2 * side]
            total[place, tile_last] += got_corners[got, 2 * side + 1]

        old = image[...]
        new = old - TAU * total[middle, :]
        if step < ITERS - 1:
            image[...] = new
            following = bars.at[step + 1]
            following[middle, :] = 2.0 * new - old
            exchange = copies(turn + 2, following, image_low, image_high)
            start_copies(exchange)
            wait_copies(exchange)
        else:
            restored_ref[...] = pltpu.roll(new, wide - half, axis=1)[:, :cols]


def per_device(observed, psf_table, psf_index, start_image, blur_dual, tv_dual):
    kernel_size = psf_table.shape[1]
    rows, cols = observed.shape
    patches = psf_index.shape[1]
    tiles = patches + 1
    wide = tiles * LANES
    turns = 2 * ITERS
    whole = pl.BlockSpec(memory_space=pltpu.VMEM)
    deep = GROUP * LANES
    weight = pltpu.VMEM((patches, deep, 2 * LANES), jnp.bfloat16)
    f32 = jnp.float32
    return pl.pallas_call(
        functools.partial(body, kernel_size),
        out_shape=(
            jax.ShapeDtypeStruct((rows, cols), f32),
            jax.ShapeDtypeStruct((rows, cols), f32),
        ),
        in_specs=[pl.BlockSpec(memory_space=pltpu.SMEM)] + [whole] * 5,
        out_specs=(whole, whole),
        scratch_shapes=[
            pltpu.VMEM((patches, 2 * GROUP, LANES), f32),
            pltpu.VMEM((patches, 2 * GROUP, LANES), f32),
            weight,
            weight,
            weight,
            weight,
            pltpu.VMEM((tiles, rows + GROUP, deep), jnp.bfloat16),
            pltpu.VMEM((rows + 2 * GROUP, cols), f32),
            pltpu.VMEM((ITERS, rows + 2 * GROUP, wide), f32),
            pltpu.VMEM((ITERS, rows + 2 * GROUP, wide), f32),
            pltpu.VMEM((rows, wide), f32),
            pltpu.VMEM((2, rows, wide), f32),
            pltpu.VMEM((turns, 2, GROUP, wide), f32),
            pltpu.VMEM((turns, 2, rows, LANES), f32),
            pltpu.VMEM((turns, 4, GROUP, LANES), f32),
            pltpu.SemaphoreType.DMA((turns, 8)),
            pltpu.SemaphoreType.DMA((turns, 8)),
        ],
        compiler_params=pltpu.CompilerParams(
            collective_id=0, has_side_effects=True, vmem_limit_bytes=60 * 1024 * 1024
        ),
    )(psf_index, observed, psf_table, start_image, blur_dual, tv_dual)


def solution(mesh):
    placed = (
        P("row", "col"),
        P(),
        P("row", "col"),
        P("row", "col"),
        P("row", "col"),
        P(None, "row", "col"),
    )
    return jax.shard_map(
        per_device,
        mesh=mesh,
        in_specs=placed,
        out_specs=(P("row", "col"), P("row", "col")),
        check_vma=False,
    )
```

```python
import functools

import jax
import jax.numpy as jnp
from jax import lax
from jax.experimental import pallas as pl
from jax.experimental.pallas import tpu as pltpu
from jax.sharding import PartitionSpec as P

ITERS = 2
SIGMA = 0.15
TAU = 0.6
TV_WEIGHT = 0.5
LANES = 128
GROUP = 16
MESH = pl.DeviceIdType.MESH

DIRECTIONS = ((-1, 0), (1, 0), (0, -1), (0, 1), (-1, -1), (-1, 1), (1, -1), (1, 1))
UP, DOWN, LEFT, RIGHT, UP_LEFT, UP_RIGHT, DOWN_LEFT, DOWN_RIGHT = range(8)
OPPOSITE = (DOWN, UP, RIGHT, LEFT, DOWN_RIGHT, DOWN_LEFT, UP_RIGHT, UP_LEFT)


def body(
    kernel_size,
    index_ref,
    observed_hbm,
    table_hbm,
    start_hbm,
    dual_hbm,
    tv_hbm,
    restored_hbm,
    dual_out_hbm,
    observed_ref,
    table_ref,
    start_ref,
    tv_ref,
    restored_ref,
    dual_out_ref,
    taps,
    taps_back,
    weights,
    weights_rest,
    adjoint,
    adjoint_rest,
    stack,
    padded_dual,
    bars,
    sums,
    image,
    tv,
    got_rows,
    got_cols,
    got_corners,
    sent_cols,
    send_sem,
    recv_sem,
    load_sem,
):
    half = kernel_size // 2
    rows, cols = observed_ref.shape
    patches = index_ref.shape[1]
    tiles = patches + 1
    wide = tiles * LANES
    tall = rows + 2 * GROUP
    reach = rows + GROUP
    last = wide - LANES
    row, col = lax.axis_index("row"), lax.axis_index("col")
    row_count, col_count = lax.axis_size("row"), lax.axis_size("col")

    def there(d):
        r, c = row + DIRECTIONS[d][0], col + DIRECTIONS[d][1]
        return (r >= 0) & (r < row_count) & (c >= 0) & (c < col_count)

    def device(d):
        return (row + DIRECTIONS[d][0], col + DIRECTIONS[d][1])

    loads = [
        pltpu.make_async_copy(source, target, load_sem.at[i])
        for i, (source, target) in enumerate(
            (
                (start_hbm, start_ref),
                (table_hbm, table_ref),
                (tv_hbm, tv_ref),
                (dual_hbm, dual_out_ref),
                (observed_hbm, observed_ref),
            )
        )
    ]
    for load in loads:
        load.start()

    got_rows[...] = jnp.zeros_like(got_rows)
    got_cols[...] = jnp.zeros_like(got_cols)
    got_corners[...] = jnp.zeros_like(got_corners)

    barrier = pltpu.get_barrier_semaphore()
    for d in range(8):

        @pl.when(there(d))
        def _():
            pl.semaphore_signal(barrier, inc=1, device_id=device(d), device_id_type=MESH)

    lane = lax.broadcasted_iota(jnp.int32, (1, LANES), 1)
    lane_wide = lax.broadcasted_iota(jnp.int32, (1, wide), 1)
    row_id = lax.broadcasted_iota(jnp.int32, (rows, 1), 0)
    own_lane = (lane_wide >= half) & (lane_wide < half + cols)
    keep_rows = (row_id < rows - 1) | (row < row_count - 1)
    keep_cols = (lane_wide < half + cols - 1) | (col < col_count - 1)

    def shifted(value):
        full = jnp.concatenate([value, jnp.zeros((rows, LANES), jnp.float32)], axis=1)
        return pltpu.roll(full, half, axis=1)

    loads[0].wait()
    start = shifted(start_ref[...])
    image[...] = start
    bars[0, :GROUP, :] = jnp.zeros((GROUP, wide), jnp.float32)
    bars[0, GROUP : GROUP + rows, :] = start
    bars[0, GROUP + rows :, :] = jnp.zeros((GROUP, wide), jnp.float32)

    tall_peers = (row > 0).astype(jnp.int32) + (row < row_count - 1).astype(jnp.int32)
    wide_peers = (col > 0).astype(jnp.int32) + (col < col_count - 1).astype(jnp.int32)
    pl.semaphore_wait(barrier, (tall_peers + 1) * (wide_peers + 1) - 1)

    inner = pl.ds(GROUP, rows)

    def copies(turn, source, low, high):
        row_part = {-1: low, 0: inner, 1: high}
        col_part = {-1: pl.ds(0, LANES), 0: pl.ds(0, wide), 1: pl.ds(last, LANES)}
        result = []
        for d, (dr, dc) in enumerate(DIRECTIONS):
            back = OPPOSITE[d]
            if d in (UP, DOWN):
                target = got_rows.at[turn, back - UP]
            elif d in (LEFT, RIGHT):
                target = got_cols.at[turn, back - LEFT]
            else:
                target = got_corners.at[turn, back - UP_LEFT]
            if d in (LEFT, RIGHT):
                origin = sent_cols.at[turn, d - LEFT]
            else:
                origin = source.at[row_part[dr], col_part[dc]]
            send = pltpu.make_async_remote_copy(
                src_ref=origin,
                dst_ref=target,
                send_sem=send_sem.at[turn, d],
                recv_sem=recv_sem.at[turn, back],
                device_id=device(d),
                device_id_type=MESH,
            )
            arrive = pltpu.make_async_remote_copy(
                src_ref=origin,
                dst_ref=(
                    got_rows.at[turn, d - UP]
                    if d in (UP, DOWN)
                    else got_cols.at[turn, d - LEFT]
                    if d in (LEFT, RIGHT)
                    else got_corners.at[turn, d - UP_LEFT]
                ),
                send_sem=send_sem.at[turn, d],
                recv_sem=recv_sem.at[turn, d],
                device_id=device(d),
                device_id_type=MESH,
            )
            result.append((send, arrive))
        return result

    def start_copies(made, which):
        for d in which:

            @pl.when(there(d))
            def _():
                made[d][0].start()

    def wait_copies(made, which):
        for d in which:

            @pl.when(there(d))
            def _():
                made[d][0].wait_send()
                made[d][1].wait_recv()

    lane_group = lane // GROUP
    groups = rows // GROUP

    def pack(source, first, offset, target):
        packed = jnp.zeros((GROUP, LANES), jnp.float32)
        for g in range(groups):
            part = source[GROUP + g * GROUP : 2 * GROUP + g * GROUP, first : first + LANES]
            moved = pltpu.roll(part, (g * GROUP - offset) % LANES, axis=1)
            packed = jnp.where(lane_group == g, moved, packed)
        target[...] = packed

    def unpack(packed, offset):
        return jnp.concatenate(
            [pltpu.roll(packed, (offset - g * GROUP) % LANES, axis=1) for g in range(groups)],
            axis=0,
        )

    near, far = (UP, DOWN), (LEFT, RIGHT, UP_LEFT, UP_RIGHT, DOWN_LEFT, DOWN_RIGHT)

    image_low, image_high = pl.ds(GROUP, GROUP), pl.ds(rows, GROUP)
    sums_low, sums_high = pl.ds(0, GROUP), pl.ds(GROUP + rows, GROUP)

    pack(bars.at[0], 0, half, sent_cols.at[0, 0])
    pack(bars.at[0], last, 0, sent_cols.at[0, 1])
    exchange = copies(0, bars.at[0], image_low, image_high)
    start_copies(exchange, far + near)

    padded_dual[...] = jnp.zeros_like(padded_dual)
    turned = lax.broadcasted_iota(jnp.int32, (LANES, LANES), 0)
    column = lax.broadcasted_iota(jnp.int32, (LANES, LANES), 1)
    reverse = (((turned + column) == LANES) | ((turned + column) == 0)).astype(jnp.bfloat16)
    entries = table_ref.shape[2]
    slot = lax.broadcasted_iota(jnp.int32, (8, entries), 0)
    entry = lax.broadcasted_iota(jnp.int32, (8, entries), 1)
    chosen = jnp.zeros((8, entries), jnp.float32)
    for patch in range(patches):
        hit = (slot == patch) & (entry == index_ref[0, patch])
        chosen = jnp.where(hit, 1.0, chosen)
    chosen = chosen.astype(jnp.bfloat16)
    taps[...] = jnp.zeros_like(taps)
    loads[1].wait()
    for tap_row in range(kernel_size):
        taps[tap_row, :, :kernel_size] = lax.dot_general(
            chosen,
            table_ref[tap_row],
            (((1,), (1,)), ((), ())),
            preferred_element_type=jnp.float32,
        )
    raw = taps[...]
    weight_sum = jnp.sum(jnp.sum(raw, axis=0), axis=1, keepdims=True)
    used = lax.broadcasted_iota(jnp.int32, (8, 1), 0) < patches
    normed = (raw / jnp.where(used, weight_sum, 1.0)[None]).astype(jnp.bfloat16)
    taps[...] = normed.astype(jnp.float32)
    taps_back[...] = jnp.dot(
        normed.reshape(2 * GROUP * 8, LANES), reverse, preferred_element_type=jnp.float32
    ).reshape(2 * GROUP, 8, LANES)

    def circulant(base):
        return pltpu.roll(
            jnp.broadcast_to(base, (LANES, LANES)), 0, axis=1, stride=1, stride_axis=0
        )

    below_diagonal = column <= turned
    above_diagonal = column >= turned

    def build(step, carry):
        patch = step // GROUP
        shift = step % GROUP
        here = pl.ds(pl.multiple_of(shift * LANES, LANES), LANES)
        for n in range(2):
            span = pl.ds(n * LANES, LANES)
            base = taps_back[n * GROUP + shift, pl.ds(patch, 1), :]
            full = circulant(base)
            weights[patch, here, span] = jnp.where(below_diagonal, full, 0.0).astype(jnp.bfloat16)
            weights_rest[patch, here, span] = jnp.where(below_diagonal, 0.0, full).astype(
                jnp.bfloat16
            )
            base = taps[n * GROUP + GROUP - 1 - shift, pl.ds(patch, 1), :]
            full = circulant(base)
            adjoint[patch, here, span] = jnp.where(above_diagonal, full, 0.0).astype(jnp.bfloat16)
            adjoint_rest[patch, here, span] = jnp.where(above_diagonal, 0.0, full).astype(
                jnp.bfloat16
            )
        return carry

    lax.fori_loop(0, patches * GROUP, build, 0)

    loads[2].wait()
    tv[0] = shifted(tv_ref[0])
    tv[1] = shifted(tv_ref[1])
    loads[3].wait()
    loads[4].wait()

    middle = pl.ds(GROUP, rows)
    tile_first, tile_last = pl.ds(0, LANES), pl.ds(last, LANES)
    in_left = lane < half
    top, bottom = pl.ds(0, GROUP), pl.ds(GROUP + rows, GROUP)
    dual_store = pltpu.make_async_copy(dual_out_ref, dual_out_hbm, load_sem.at[0])
    image_store = pltpu.make_async_copy(restored_ref, restored_hbm, load_sem.at[1])

    for step in range(ITERS):
        turn = 2 * step
        bar = bars.at[step]
        total = sums.at[step]

        wait_copies(exchange, near)
        bar[top, :] = got_rows[turn, 0]
        bar[bottom, :] = got_rows[turn, 1]

        def stack_bar(tile, carry):
            here = pl.ds(pl.multiple_of(tile * LANES, LANES), LANES)
            for shift in range(GROUP):
                stack[tile, :, shift * LANES : (shift + 1) * LANES] = bar[
                    pl.ds(shift + 1, reach), here
                ].astype(jnp.bfloat16)
            return carry

        lax.fori_loop(1, tiles - 1, stack_bar, 0)

        def blur(patch, carry):
            here = pl.ds(pl.multiple_of(patch * LANES, LANES), LANES)
            both = jnp.dot(stack[patch], weights[patch], preferred_element_type=jnp.float32)
            both += jnp.dot(
                stack[patch + 1], weights_rest[patch], preferred_element_type=jnp.float32
            )
            blurred = both[:rows, :LANES] + both[GROUP:, LANES:]
            dual = (dual_out_ref[:, here] + SIGMA * (blurred - observed_ref[:, here])) / (
                1.0 + SIGMA
            )
            dual_out_ref[:, here] = dual
            padded_dual[GROUP : GROUP + rows, here] = dual
            return carry

        lax.fori_loop(1, patches - 1, blur, 0)

        wait_copies(exchange, far)
        bar[middle, tile_first] = jnp.where(
            in_left, unpack(got_cols[turn, 0], 0), bar[middle, tile_first]
        )
        in_right = (lane >= half) & (lane < half + GROUP)
        bar[middle, tile_last] = jnp.where(
            in_left,
            bar[middle, tile_last],
            jnp.where(in_right, unpack(got_cols[turn, 1], half), 0.0),
        )
        for side, place in ((0, top), (1, bottom)):
            bar[place, tile_first] = jnp.where(
                in_left, got_corners[turn, 2 * side], got_rows[turn, side, :, :LANES]
            )
            bar[place, tile_last] = jnp.where(
                in_left, got_rows[turn, side, :, last:], got_corners[turn, 2 * side + 1]
            )
        stack_bar(0, 0)
        stack_bar(tiles - 1, 0)
        blur(0, 0)
        blur(patches - 1, 0)
        if step == ITERS - 1:
            dual_store.start()

        now = bar[middle, :]
        grad_rows = jnp.where(keep_rows, bar[pl.ds(GROUP + 1, rows), :] - now, 0.0)
        grad_cols = jnp.where(keep_cols, pltpu.roll(now, wide - 1, axis=1) - now, 0.0)
        moved_rows = tv[0] + SIGMA * grad_rows
        moved_cols = tv[1] + SIGMA * grad_cols
        shrink = jnp.maximum(
            1.0, jnp.sqrt(moved_rows * moved_rows + moved_cols * moved_cols) / TV_WEIGHT
        )
        new_rows = moved_rows / shrink
        new_cols = moved_cols / shrink
        tv[0] = new_rows
        tv[1] = new_cols
        masked_rows = jnp.where(keep_rows & own_lane, new_rows, 0.0)
        masked_cols = jnp.where(keep_cols & own_lane, new_cols, 0.0)
        total[top, :] = jnp.zeros((GROUP, wide), jnp.float32)
        total[bottom, :] = jnp.zeros((GROUP, wide), jnp.float32)
        total[middle, :] = pltpu.roll(masked_cols, 1, axis=1) - masked_cols - masked_rows
        total[pl.ds(GROUP + 1, rows), :] += masked_rows

        def stack_dual(patch, carry):
            here = pl.ds(pl.multiple_of(patch * LANES, LANES), LANES)
            for shift in range(GROUP):
                stack[patch, :, shift * LANES : (shift + 1) * LANES] = padded_dual[
                    pl.ds(shift, reach), here
                ].astype(jnp.bfloat16)
            return carry

        lax.fori_loop(0, patches, stack_dual, 0)

        def put(tile, both):
            here = pl.ds(pl.multiple_of(tile * LANES, LANES), LANES)
            total[:GROUP, here] += both[:GROUP, :LANES]
            total[pl.ds(GROUP, rows), here] += both[GROUP:, :LANES] + both[:rows, LANES:]
            total[pl.ds(GROUP + rows, GROUP), here] += both[rows:, LANES:]

        put(0, jnp.dot(stack[0], adjoint[0], preferred_element_type=jnp.float32))

        def spread(tile, carry):
            both = jnp.dot(stack[tile], adjoint[tile], preferred_element_type=jnp.float32)
            both += jnp.dot(
                stack[tile - 1], adjoint_rest[tile - 1], preferred_element_type=jnp.float32
            )
            put(tile, both)
            return carry

        put(
            patches,
            jnp.dot(
                stack[patches - 1], adjoint_rest[patches - 1], preferred_element_type=jnp.float32
            ),
        )
        pack(total, 0, 0, sent_cols.at[turn + 1, 0])
        pack(total, last, half, sent_cols.at[turn + 1, 1])
        exchange = copies(turn + 1, total, sums_low, sums_high)
        start_copies(exchange, far)
        lax.fori_loop(1, patches, spread, 0)
        start_copies(exchange, near)
        wait_copies(exchange, near + far)

        got = turn + 1
        in_right = (lane >= half) & (lane < half + GROUP)
        from_left = unpack(got_cols[got, 0], half)
        total[middle, tile_first] += jnp.where(in_right, from_left, 0.0)
        from_right = unpack(got_cols[got, 1], 0)
        total[middle, tile_last] += jnp.where(lane < GROUP, from_right, 0.0)
        for side, place in ((0, pl.ds(GROUP, GROUP)), (1, pl.ds(rows, GROUP))):
            total[place, :] += got_rows[got, side]
            total[place, tile_first] += got_corners[got, 2 * side]
            total[place, tile_last] += got_corners[got, 2 * side + 1]

        old = image[...]
        new = old - TAU * total[middle, :]
        if step < ITERS - 1:
            image[...] = new
            following = bars.at[step + 1]
            following[middle, :] = 2.0 * new - old
            pack(following, 0, half, sent_cols.at[turn + 2, 0])
            pack(following, last, 0, sent_cols.at[turn + 2, 1])
            exchange = copies(turn + 2, following, image_low, image_high)
            start_copies(exchange, far + near)
        else:
            restored_ref[...] = pltpu.roll(new, wide - half, axis=1)[:, :cols]
            image_store.start()
            dual_store.wait()
            image_store.wait()


def per_device(observed, psf_table, psf_index, start_image, blur_dual, tv_dual):
    kernel_size = psf_table.shape[1]
    rows, cols = observed.shape
    patches = psf_index.shape[1]
    tiles = patches + 1
    wide = tiles * LANES
    turns = 2 * ITERS
    table = psf_table.transpose(1, 2, 0)
    deep = GROUP * LANES
    weight = pltpu.VMEM((patches, deep, 2 * LANES), jnp.bfloat16)
    f32 = jnp.float32
    anywhere = pl.BlockSpec(memory_space=pl.ANY)
    return pl.pallas_call(
        functools.partial(body, kernel_size),
        out_shape=(
            jax.ShapeDtypeStruct((rows, cols), f32),
            jax.ShapeDtypeStruct((rows, cols), f32),
        ),
        in_specs=[pl.BlockSpec(memory_space=pltpu.SMEM)] + [anywhere] * 5,
        out_specs=(anywhere, anywhere),
        scratch_shapes=[
            pltpu.VMEM((rows, cols), f32),
            pltpu.VMEM(table.shape, table.dtype),
            pltpu.VMEM((rows, cols), f32),
            pltpu.VMEM((2, rows, cols), f32),
            pltpu.VMEM((rows, cols), f32),
            pltpu.VMEM((rows, cols), f32),
            pltpu.VMEM((2 * GROUP, 8, LANES), f32),
            pltpu.VMEM((2 * GROUP, 8, LANES), f32),
            weight,
            weight,
            weight,
            weight,
            pltpu.VMEM((tiles, rows + GROUP, deep), jnp.bfloat16),
            pltpu.VMEM((rows + 2 * GROUP, cols), f32),
            pltpu.VMEM((ITERS, rows + 2 * GROUP, wide), f32),
            pltpu.VMEM((ITERS, rows + 2 * GROUP, wide), f32),
            pltpu.VMEM((rows, wide), f32),
            pltpu.VMEM((2, rows, wide), f32),
            pltpu.VMEM((turns, 2, GROUP, wide), f32),
            pltpu.VMEM((turns, 2, GROUP, LANES), f32),
            pltpu.VMEM((turns, 4, GROUP, LANES), f32),
            pltpu.VMEM((turns, 2, GROUP, LANES), f32),
            pltpu.SemaphoreType.DMA((turns, 8)),
            pltpu.SemaphoreType.DMA((turns, 8)),
            pltpu.SemaphoreType.DMA((5,)),
        ],
        compiler_params=pltpu.CompilerParams(
            collective_id=0, has_side_effects=True, vmem_limit_bytes=60 * 1024 * 1024
        ),
    )(psf_index, observed, table, start_image, blur_dual, tv_dual)


def solution(mesh):
    placed = (
        P("row", "col"),
        P(),
        P("row", "col"),
        P("row", "col"),
        P("row", "col"),
        P(None, "row", "col"),
    )
    return jax.shard_map(
        per_device,
        mesh=mesh,
        in_specs=placed,
        out_specs=(P("row", "col"), P("row", "col")),
        check_vma=False,
    )
```

```python
import functools

import jax
import jax.numpy as jnp
from jax import lax
from jax.experimental import pallas as pl
from jax.experimental.pallas import tpu as pltpu
from jax.sharding import PartitionSpec as P

ITERS = 2
SIGMA = 0.15
TAU = 0.6
TV_WEIGHT = 0.5
LANES = 128
GROUP = 16
MESH = pl.DeviceIdType.MESH

DIRECTIONS = ((-1, 0), (1, 0), (0, -1), (0, 1), (-1, -1), (-1, 1), (1, -1), (1, 1))
UP, DOWN, LEFT, RIGHT, UP_LEFT, UP_RIGHT, DOWN_LEFT, DOWN_RIGHT = range(8)
OPPOSITE = (DOWN, UP, RIGHT, LEFT, DOWN_RIGHT, DOWN_LEFT, UP_RIGHT, UP_LEFT)


def body(
    kernel_size,
    index_ref,
    observed_hbm,
    table_hbm,
    start_hbm,
    dual_hbm,
    tv_hbm,
    restored_hbm,
    dual_out_hbm,
    observed_ref,
    table_ref,
    start_ref,
    tv_ref,
    restored_ref,
    dual_out_ref,
    taps,
    taps_back,
    weights,
    weights_rest,
    adjoint,
    adjoint_rest,
    stack,
    stack_back,
    padded_dual,
    bars,
    sums,
    image,
    tv,
    got_rows,
    got_cols,
    got_corners,
    sent_cols,
    send_sem,
    recv_sem,
    load_sem,
):
    half = kernel_size // 2
    rows, cols = observed_ref.shape
    patches = index_ref.shape[1]
    tiles = patches + 1
    wide = tiles * LANES
    tall = rows + 2 * GROUP
    reach = rows + GROUP
    last = wide - LANES
    row, col = lax.axis_index("row"), lax.axis_index("col")
    row_count, col_count = lax.axis_size("row"), lax.axis_size("col")

    def there(d):
        r, c = row + DIRECTIONS[d][0], col + DIRECTIONS[d][1]
        return (r >= 0) & (r < row_count) & (c >= 0) & (c < col_count)

    def device(d):
        return (row + DIRECTIONS[d][0], col + DIRECTIONS[d][1])

    loads = [
        pltpu.make_async_copy(source, target, load_sem.at[i])
        for i, (source, target) in enumerate(
            (
                (start_hbm, start_ref),
                (table_hbm, table_ref),
                (tv_hbm, tv_ref),
                (dual_hbm, dual_out_ref),
                (observed_hbm, observed_ref),
            )
        )
    ]
    for load in loads:
        load.start()

    got_rows[...] = jnp.zeros_like(got_rows)
    got_cols[...] = jnp.zeros_like(got_cols)
    got_corners[...] = jnp.zeros_like(got_corners)

    barrier = pltpu.get_barrier_semaphore()
    for d in range(8):

        @pl.when(there(d))
        def _():
            pl.semaphore_signal(barrier, inc=1, device_id=device(d), device_id_type=MESH)

    lane = lax.broadcasted_iota(jnp.int32, (1, LANES), 1)
    lane_wide = lax.broadcasted_iota(jnp.int32, (1, wide), 1)
    row_id = lax.broadcasted_iota(jnp.int32, (rows, 1), 0)
    own_lane = (lane_wide >= half) & (lane_wide < half + cols)
    keep_rows = (row_id < rows - 1) | (row < row_count - 1)
    keep_cols = (lane_wide < half + cols - 1) | (col < col_count - 1)

    def shifted(value):
        full = jnp.concatenate([value, jnp.zeros((rows, LANES), jnp.float32)], axis=1)
        return pltpu.roll(full, half, axis=1)

    loads[0].wait()
    start = shifted(start_ref[...])
    image[...] = start
    bars[0, :GROUP, :] = jnp.zeros((GROUP, wide), jnp.float32)
    bars[0, GROUP : GROUP + rows, :] = start
    bars[0, GROUP + rows :, :] = jnp.zeros((GROUP, wide), jnp.float32)

    tall_peers = (row > 0).astype(jnp.int32) + (row < row_count - 1).astype(jnp.int32)
    wide_peers = (col > 0).astype(jnp.int32) + (col < col_count - 1).astype(jnp.int32)
    pl.semaphore_wait(barrier, (tall_peers + 1) * (wide_peers + 1) - 1)

    inner = pl.ds(GROUP, rows)

    def copies(turn, source, low, high):
        row_part = {-1: low, 0: inner, 1: high}
        col_part = {-1: pl.ds(0, LANES), 0: pl.ds(0, wide), 1: pl.ds(last, LANES)}
        result = []
        for d, (dr, dc) in enumerate(DIRECTIONS):
            back = OPPOSITE[d]
            if d in (UP, DOWN):
                target = got_rows.at[turn, back - UP]
            elif d in (LEFT, RIGHT):
                target = got_cols.at[turn, back - LEFT]
            else:
                target = got_corners.at[turn, back - UP_LEFT]
            if d in (LEFT, RIGHT):
                origin = sent_cols.at[turn, d - LEFT]
            else:
                origin = source.at[row_part[dr], col_part[dc]]
            send = pltpu.make_async_remote_copy(
                src_ref=origin,
                dst_ref=target,
                send_sem=send_sem.at[turn, d],
                recv_sem=recv_sem.at[turn, back],
                device_id=device(d),
                device_id_type=MESH,
            )
            arrive = pltpu.make_async_remote_copy(
                src_ref=origin,
                dst_ref=(
                    got_rows.at[turn, d - UP]
                    if d in (UP, DOWN)
                    else got_cols.at[turn, d - LEFT]
                    if d in (LEFT, RIGHT)
                    else got_corners.at[turn, d - UP_LEFT]
                ),
                send_sem=send_sem.at[turn, d],
                recv_sem=recv_sem.at[turn, d],
                device_id=device(d),
                device_id_type=MESH,
            )
            result.append((send, arrive))
        return result

    def start_copies(made, which):
        for d in which:

            @pl.when(there(d))
            def _():
                made[d][0].start()

    def wait_copies(made, which):
        for d in which:

            @pl.when(there(d))
            def _():
                made[d][0].wait_send()
                made[d][1].wait_recv()

    lane_group = lane // GROUP
    groups = rows // GROUP

    def pack(source, first, offset, target):
        packed = jnp.zeros((GROUP, LANES), jnp.float32)
        for g in range(groups):
            part = source[GROUP + g * GROUP : 2 * GROUP + g * GROUP, first : first + LANES]
            moved = pltpu.roll(part, (g * GROUP - offset) % LANES, axis=1)
            packed = jnp.where(lane_group == g, moved, packed)
        target[...] = packed

    def unpack(packed, offset):
        return jnp.concatenate(
            [pltpu.roll(packed, (offset - g * GROUP) % LANES, axis=1) for g in range(groups)],
            axis=0,
        )

    near, far = (UP, DOWN), (LEFT, RIGHT, UP_LEFT, UP_RIGHT, DOWN_LEFT, DOWN_RIGHT)

    image_low, image_high = pl.ds(GROUP, GROUP), pl.ds(rows, GROUP)
    sums_low, sums_high = pl.ds(0, GROUP), pl.ds(GROUP + rows, GROUP)

    pack(bars.at[0], 0, half, sent_cols.at[0, 0])
    pack(bars.at[0], last, 0, sent_cols.at[0, 1])
    exchange = copies(0, bars.at[0], image_low, image_high)
    start_copies(exchange, near + far)

    padded_dual[...] = jnp.zeros_like(padded_dual)
    turned = lax.broadcasted_iota(jnp.int32, (LANES, LANES), 0)
    column = lax.broadcasted_iota(jnp.int32, (LANES, LANES), 1)
    reverse = (((turned + column) == LANES) | ((turned + column) == 0)).astype(jnp.bfloat16)
    entries = table_ref.shape[2]
    slot = lax.broadcasted_iota(jnp.int32, (8, entries), 0)
    entry = lax.broadcasted_iota(jnp.int32, (8, entries), 1)
    chosen = jnp.zeros((8, entries), jnp.float32)
    for patch in range(patches):
        hit = (slot == patch) & (entry == index_ref[0, patch])
        chosen = jnp.where(hit, 1.0, chosen)
    chosen = chosen.astype(jnp.bfloat16)
    taps[...] = jnp.zeros_like(taps)
    loads[1].wait()
    for tap_row in range(kernel_size):
        taps[tap_row, :, :kernel_size] = lax.dot_general(
            chosen,
            table_ref[tap_row],
            (((1,), (1,)), ((), ())),
            preferred_element_type=jnp.float32,
        )
    raw = taps[...]
    weight_sum = jnp.sum(jnp.sum(raw, axis=0), axis=1, keepdims=True)
    used = lax.broadcasted_iota(jnp.int32, (8, 1), 0) < patches
    normed = (raw / jnp.where(used, weight_sum, 1.0)[None]).astype(jnp.bfloat16)
    taps[...] = normed.astype(jnp.float32)
    taps_back[...] = jnp.dot(
        normed.reshape(2 * GROUP * 8, LANES), reverse, preferred_element_type=jnp.float32
    ).reshape(2 * GROUP, 8, LANES)

    def circulant(base):
        return pltpu.roll(
            jnp.broadcast_to(base, (LANES, LANES)), 0, axis=1, stride=1, stride_axis=0
        )

    below_diagonal = column <= turned
    above_diagonal = column >= turned

    def build(step, carry):
        patch = step // GROUP
        shift = step % GROUP
        here = pl.ds(pl.multiple_of(shift * LANES, LANES), LANES)
        for n in range(2):
            span = pl.ds(n * LANES, LANES)
            base = taps_back[n * GROUP + shift, pl.ds(patch, 1), :]
            full = circulant(base)
            weights[patch, here, span] = jnp.where(below_diagonal, full, 0.0).astype(jnp.bfloat16)
            weights_rest[patch, here, span] = jnp.where(below_diagonal, 0.0, full).astype(
                jnp.bfloat16
            )
            base = taps[n * GROUP + GROUP - 1 - shift, pl.ds(patch, 1), :]
            full = circulant(base)
            adjoint[patch, here, span] = jnp.where(above_diagonal, full, 0.0).astype(jnp.bfloat16)
            adjoint_rest[patch, here, span] = jnp.where(above_diagonal, 0.0, full).astype(
                jnp.bfloat16
            )
        return carry

    lax.fori_loop(0, patches * GROUP, build, 0, unroll=4)

    loads[2].wait()
    tv[0] = shifted(tv_ref[0])
    tv[1] = shifted(tv_ref[1])
    loads[3].wait()
    loads[4].wait()

    middle = pl.ds(GROUP, rows)
    tile_first, tile_last = pl.ds(0, LANES), pl.ds(last, LANES)
    in_left = lane < half
    top, bottom = pl.ds(0, GROUP), pl.ds(GROUP + rows, GROUP)
    dual_store = pltpu.make_async_copy(dual_out_ref, dual_out_hbm, load_sem.at[0])
    image_store = pltpu.make_async_copy(restored_ref, restored_hbm, load_sem.at[1])

    for step in range(ITERS):
        turn = 2 * step
        bar = bars.at[step]
        total = sums.at[step]

        wait_copies(exchange, near)
        bar[top, :] = got_rows[turn, 0]
        bar[bottom, :] = got_rows[turn, 1]

        def stack_bar(tile, carry):
            here = pl.ds(pl.multiple_of(tile * LANES, LANES), LANES)
            for shift in range(GROUP):
                stack[tile, :, shift * LANES : (shift + 1) * LANES] = bar[
                    pl.ds(shift + 1, reach), here
                ].astype(jnp.bfloat16)
            return carry

        lax.fori_loop(1, tiles - 1, stack_bar, 0)

        def blur(patch, carry):
            here = pl.ds(pl.multiple_of(patch * LANES, LANES), LANES)
            both = jnp.dot(stack[patch], weights[patch], preferred_element_type=jnp.float32)
            both += jnp.dot(
                stack[patch + 1], weights_rest[patch], preferred_element_type=jnp.float32
            )
            blurred = both[:rows, :LANES] + both[GROUP:, LANES:]
            dual = (dual_out_ref[:, here] + SIGMA * (blurred - observed_ref[:, here])) / (
                1.0 + SIGMA
            )
            dual_out_ref[:, here] = dual
            padded_dual[GROUP : GROUP + rows, here] = dual
            return carry

        lax.fori_loop(1, patches - 1, blur, 0)

        wait_copies(exchange, far)
        bar[middle, tile_first] = jnp.where(
            in_left, unpack(got_cols[turn, 0], 0), bar[middle, tile_first]
        )
        in_right = (lane >= half) & (lane < half + GROUP)
        bar[middle, tile_last] = jnp.where(
            in_left,
            bar[middle, tile_last],
            jnp.where(in_right, unpack(got_cols[turn, 1], half), 0.0),
        )
        for side, place in ((0, top), (1, bottom)):
            bar[place, tile_first] = jnp.where(
                in_left, got_corners[turn, 2 * side], got_rows[turn, side, :, :LANES]
            )
            bar[place, tile_last] = jnp.where(
                in_left, got_rows[turn, side, :, last:], got_corners[turn, 2 * side + 1]
            )
        stack_bar(0, 0)
        stack_bar(tiles - 1, 0)
        def stack_dual(patch, carry):
            here = pl.ds(pl.multiple_of(patch * LANES, LANES), LANES)
            for shift in range(GROUP):
                stack_back[patch, :, shift * LANES : (shift + 1) * LANES] = padded_dual[
                    pl.ds(shift, reach), here
                ].astype(jnp.bfloat16)
            return carry

        blur(0, 0)
        blur(patches - 1, 0)
        for patch in range(1, patches - 1):
            stack_dual(patch, 0)
        if step == ITERS - 1:
            dual_store.start()

        now = bar[middle, :]
        grad_rows = jnp.where(keep_rows, bar[pl.ds(GROUP + 1, rows), :] - now, 0.0)
        grad_cols = jnp.where(keep_cols, pltpu.roll(now, wide - 1, axis=1) - now, 0.0)
        moved_rows = tv[0] + SIGMA * grad_rows
        moved_cols = tv[1] + SIGMA * grad_cols
        shrink = jnp.maximum(
            1.0, jnp.sqrt(moved_rows * moved_rows + moved_cols * moved_cols) / TV_WEIGHT
        )
        new_rows = moved_rows / shrink
        new_cols = moved_cols / shrink
        tv[0] = new_rows
        tv[1] = new_cols
        masked_rows = jnp.where(keep_rows & own_lane, new_rows, 0.0)
        masked_cols = jnp.where(keep_cols & own_lane, new_cols, 0.0)
        total[top, :] = jnp.zeros((GROUP, wide), jnp.float32)
        total[bottom, :] = jnp.zeros((GROUP, wide), jnp.float32)
        total[middle, :] = pltpu.roll(masked_cols, 1, axis=1) - masked_cols - masked_rows
        total[pl.ds(GROUP + 1, rows), :] += masked_rows

        stack_dual(0, 0)
        stack_dual(patches - 1, 0)

        def put(tile, both):
            here = pl.ds(pl.multiple_of(tile * LANES, LANES), LANES)
            total[:GROUP, here] += both[:GROUP, :LANES]
            total[pl.ds(GROUP, rows), here] += both[GROUP:, :LANES] + both[:rows, LANES:]
            total[pl.ds(GROUP + rows, GROUP), here] += both[rows:, LANES:]

        put(0, jnp.dot(stack_back[0], adjoint[0], preferred_element_type=jnp.float32))

        def spread(tile, carry):
            both = jnp.dot(stack_back[tile], adjoint[tile], preferred_element_type=jnp.float32)
            both += jnp.dot(
                stack_back[tile - 1], adjoint_rest[tile - 1], preferred_element_type=jnp.float32
            )
            put(tile, both)
            return carry

        put(
            patches,
            jnp.dot(
                stack_back[patches - 1], adjoint_rest[patches - 1], preferred_element_type=jnp.float32
            ),
        )
        pack(total, 0, 0, sent_cols.at[turn + 1, 0])
        pack(total, last, half, sent_cols.at[turn + 1, 1])
        exchange = copies(turn + 1, total, sums_low, sums_high)
        start_copies(exchange, far)
        lax.fori_loop(1, patches, spread, 0)
        start_copies(exchange, near)
        wait_copies(exchange, near + far)

        got = turn + 1
        in_right = (lane >= half) & (lane < half + GROUP)
        from_left = unpack(got_cols[got, 0], half)
        total[middle, tile_first] += jnp.where(in_right, from_left, 0.0)
        from_right = unpack(got_cols[got, 1], 0)
        total[middle, tile_last] += jnp.where(lane < GROUP, from_right, 0.0)
        for side, place in ((0, pl.ds(GROUP, GROUP)), (1, pl.ds(rows, GROUP))):
            total[place, :] += got_rows[got, side]
            total[place, tile_first] += got_corners[got, 2 * side]
            total[place, tile_last] += got_corners[got, 2 * side + 1]

        old = image[...]
        new = old - TAU * total[middle, :]
        if step < ITERS - 1:
            image[...] = new
            following = bars.at[step + 1]
            following[middle, :] = 2.0 * new - old
            pack(following, 0, half, sent_cols.at[turn + 2, 0])
            pack(following, last, 0, sent_cols.at[turn + 2, 1])
            exchange = copies(turn + 2, following, image_low, image_high)
            start_copies(exchange, near + far)
        else:
            restored_ref[...] = pltpu.roll(new, wide - half, axis=1)[:, :cols]
            image_store.start()
            dual_store.wait()
            image_store.wait()


def per_device(observed, psf_table, psf_index, start_image, blur_dual, tv_dual):
    kernel_size = psf_table.shape[1]
    rows, cols = observed.shape
    patches = psf_index.shape[1]
    tiles = patches + 1
    wide = tiles * LANES
    turns = 2 * ITERS
    table = psf_table.transpose(1, 2, 0)
    deep = GROUP * LANES
    weight = pltpu.VMEM((patches, deep, 2 * LANES), jnp.bfloat16)
    f32 = jnp.float32
    anywhere = pl.BlockSpec(memory_space=pl.ANY)
    return pl.pallas_call(
        functools.partial(body, kernel_size),
        out_shape=(
            jax.ShapeDtypeStruct((rows, cols), f32),
            jax.ShapeDtypeStruct((rows, cols), f32),
        ),
        in_specs=[pl.BlockSpec(memory_space=pltpu.SMEM)] + [anywhere] * 5,
        out_specs=(anywhere, anywhere),
        scratch_shapes=[
            pltpu.VMEM((rows, cols), f32),
            pltpu.VMEM(table.shape, table.dtype),
            pltpu.VMEM((rows, cols), f32),
            pltpu.VMEM((2, rows, cols), f32),
            pltpu.VMEM((rows, cols), f32),
            pltpu.VMEM((rows, cols), f32),
            pltpu.VMEM((2 * GROUP, 8, LANES), f32),
            pltpu.VMEM((2 * GROUP, 8, LANES), f32),
            weight,
            weight,
            weight,
            weight,
            pltpu.VMEM((tiles, rows + GROUP, deep), jnp.bfloat16),
            pltpu.VMEM((patches, rows + GROUP, deep), jnp.bfloat16),
            pltpu.VMEM((rows + 2 * GROUP, cols), f32),
            pltpu.VMEM((ITERS, rows + 2 * GROUP, wide), f32),
            pltpu.VMEM((ITERS, rows + 2 * GROUP, wide), f32),
            pltpu.VMEM((rows, wide), f32),
            pltpu.VMEM((2, rows, wide), f32),
            pltpu.VMEM((turns, 2, GROUP, wide), f32),
            pltpu.VMEM((turns, 2, GROUP, LANES), f32),
            pltpu.VMEM((turns, 4, GROUP, LANES), f32),
            pltpu.VMEM((turns, 2, GROUP, LANES), f32),
            pltpu.SemaphoreType.DMA((turns, 8)),
            pltpu.SemaphoreType.DMA((turns, 8)),
            pltpu.SemaphoreType.DMA((5,)),
        ],
        compiler_params=pltpu.CompilerParams(
            collective_id=0, has_side_effects=True, vmem_limit_bytes=60 * 1024 * 1024
        ),
    )(psf_index, observed, table, start_image, blur_dual, tv_dual)


def solution(mesh):
    placed = (
        P("row", "col"),
        P(),
        P("row", "col"),
        P("row", "col"),
        P("row", "col"),
        P(None, "row", "col"),
    )
    return jax.shard_map(
        per_device,
        mesh=mesh,
        in_specs=placed,
        out_specs=(P("row", "col"), P("row", "col")),
        check_vma=False,
    )
```
